32 devices in a mesh: dp: 8 (over y, x, core), mp: 4 (over z).
Axes of the slice: x: 2, y: 2, z: 4, core: 2. Of those that a mesh axis runs over, the one named last changes fastest.
Arguments:
- block_in: bfloat16 [8192, 1024], P(('dp', 'mp')), may hold values from -6 to 6
- out_grad: bfloat16 [8192, 1024], P(('dp', 'mp')), may hold values from -6 to 6
- slot_group: int32 [8], P('dp'), may hold values from 0 to 1, as said below
- decay_rate: float32 [1024], replicated, may hold values from 0.3 to 12
- norm_gain: float32 [2, 1024], replicated, may hold values from 0.1 to 1.9
- norm_gain_moment_one: float32 [2, 1024], replicated, may hold values from -0.00018310547 to 0.00018310547
- norm_gain_moment_two: float32 [2, 1024], replicated, may hold values from 1.5894572e-09 to 7.947286e-09
- short_kernel: float32 [3, 3, 1024], replicated, may hold values from -3.5 to 3.5
- short_kernel_moment_one: float32 [3, 3, 1024], replicated, may hold values from -0.00018310547 to 0.00018310547
- short_kernel_moment_two: float32 [3, 3, 1024], replicated, may hold values from 1.5894572e-09 to 7.947286e-09
- skip_bias: float32 [1024], replicated, may hold values from -6 to 6
- skip_bias_moment_one: float32 [1024], replicated, may hold values from -0.00018310547 to 0.00018310547
- skip_bias_moment_two: float32 [1024], replicated, may hold values from 1.5894572e-09 to 7.947286e-09
- filter_first: float32 [33, 64], replicated, may hold values from -1 to 1
- filter_first_moment_one: float32 [33, 64], replicated, may hold values from -0.00018310547 to 0.00018310547
- filter_first_moment_two: float32 [33, 64], replicated, may hold values from 1.5894572e-09 to 7.947286e-09
- filter_inner: float32 [2, 64, 64], replicated, may hold values from -0.75 to 0.75
- filter_inner_moment_one: float32 [2, 64, 64], replicated, may hold values from -0.00018310547 to 0.00018310547
- filter_inner_moment_two: float32 [2, 64, 64], replicated, may hold values from 1.5894572e-09 to 7.947286e-09
- filter_last: float32 [64, 1024], replicated, may hold values from -0.109375 to 0.109375
- filter_last_moment_one: float32 [64, 1024], replicated, may hold values from -0.00018310547 to 0.00018310547
- filter_last_moment_two: float32 [64, 1024], replicated, may hold values from 1.5894572e-09 to 7.947286e-09
- in_weight: float32 [3, 1024, 1024], P(None, 'mp', 'dp'), may hold values from -0.1875 to 0.1875
- in_weight_moment_one: float32 [3, 1024, 1024], P(None, 'mp', 'dp'), may hold values from -0.00018310547 to 0.00018310547
- in_weight_moment_two: float32 [3, 1024, 1024], P(None, 'mp', 'dp'), may hold values from 1.5894572e-09 to 7.947286e-09
- out_weight: float32 [1024, 1024], P('mp', 'dp'), may hold values from -0.1875 to 0.1875
- out_weight_moment_one: float32 [1024, 1024], P('mp', 'dp'), may hold values from -0.00018310547 to 0.00018310547
- out_weight_moment_two: float32 [1024, 1024], P('mp', 'dp'), may hold values from 1.5894572e-09 to 7.947286e-09
- up_weight: float32 [4096, 1024], P('mp', 'dp'), may hold values from -0.1875 to 0.1875
- up_weight_moment_one: float32 [4096, 1024], P('mp', 'dp'), may hold values from -0.00018310547 to 0.00018310547
- up_weight_moment_two: float32 [4096, 1024], P('mp', 'dp'), may hold values from 1.5894572e-09 to 7.947286e-09
- down_weight: float32 [4096, 1024], P('mp', 'dp'), may hold values from -0.09375 to 0.09375
- down_weight_moment_one: float32 [4096, 1024], P('mp', 'dp'), may hold values from -0.00018310547 to 0.00018310547
- down_weight_moment_two: float32 [4096, 1024], P('mp', 'dp'), may hold values from 1.5894572e-09 to 7.947286e-09
Outputs:
- block_out: bfloat16 [8192, 1024], P(('dp', 'mp'))
- in_grad: float32 [8192, 1024], P(('dp', 'mp'))
- grad_norm: float32 [], replicated
- norm_gain_update: float32 [2, 1024], replicated
- new_norm_gain_moment_one: float32 [2, 1024], replicated
- new_norm_gain_moment_two: float32 [2, 1024], replicated
- short_kernel_update: float32 [3, 3, 1024], replicated
- new_short_kernel_moment_one: float32 [3, 3, 1024], replicated
- new_short_kernel_moment_two: float32 [3, 3, 1024], replicated
- skip_bias_update: float32 [1024], replicated
- new_skip_bias_moment_one: float32 [1024], replicated
- new_skip_bias_moment_two: float32 [1024], replicated
- filter_first_update: float32 [33, 64], replicated
- new_filter_first_moment_one: float32 [33, 64], replicated
- new_filter_first_moment_two: float32 [33, 64], replicated
- filter_inner_update: float32 [2, 64, 64], replicated
- new_filter_inner_moment_one: float32 [2, 64, 64], replicated
- new_filter_inner_moment_two: float32 [2, 64, 64], replicated
- filter_last_update: float32 [64, 1024], replicated
- new_filter_last_moment_one: float32 [64, 1024], replicated
- new_filter_last_moment_two: float32 [64, 1024], replicated
- in_weight_update: float32 [3, 1024, 1024], P(None, 'mp', 'dp')
- new_in_weight_moment_one: float32 [3, 1024, 1024], P(None, 'mp', 'dp')
- new_in_weight_moment_two: float32 [3, 1024, 1024], P(None, 'mp', 'dp')
- out_weight_update: float32 [1024, 1024], P('mp', 'dp')
- new_out_weight_moment_one: float32 [1024, 1024], P('mp', 'dp')
- new_out_weight_moment_two: float32 [1024, 1024], P('mp', 'dp')
- up_weight_update: float32 [4096, 1024], P('mp', 'dp')
- new_up_weight_moment_one: float32 [4096, 1024], P('mp', 'dp')
- new_up_weight_moment_two: float32 [4096, 1024], P('mp', 'dp')
- down_weight_update: float32 [4096, 1024], P('mp', 'dp')
- new_down_weight_moment_one: float32 [4096, 1024], P('mp', 'dp')
- new_down_weight_moment_two: float32 [4096, 1024], P('mp', 'dp')
The draws below stay inside these ranges and needn't reach their ends.
Inputs may be any that keep to these rules, and one draw needn't show every extreme that they name: `slot_group`: 0 where a slot is one sequence of 1024 tokens, 1 where it is 4 sequences of 256 tokens; both values occur.
All inputs are finite; a program needn't handle non-finite values.
Results may differ from the reference program's by a relative error of at most 0.007.
The reference program's roundings to bfloat16 on the way count: a program that leaves them out, or rounds other values in their place, can miss the bound.
Values may be sent and summed in bfloat16 or wider, within the bound.
A program may use at most 256 MiB of HBM per device.

```python
import math
import jax
import jax.numpy as jnp
from jax import lax

D = 1024
FF = 4096
FILTER = 64
EMBED = 33
TAPS = 3
SHORT = 256
STEP = 10
SLOT = 1024
TOKENS = 8192
N_DP = 8


def draw_slot_group(key, part):
    key_one, key_two = jax.random.split(key)
    group_flags = jax.random.randint(key_one, (N_DP,), 0, 2)
    shuffled = jax.random.permutation(key_two, N_DP)
    group_flags = group_flags.at[shuffled[0]].set(0).at[shuffled[1]].set(1)
    return group_flags.astype(jnp.int32)


def block_scale(own_key, extent, cuts, least, top_value):
    loudness = 1.0
    for axis_at, parts in cuts:
        draws = jax.random.uniform(jax.random.fold_in(jax.random.fold_in(own_key, 6), axis_at), (parts,), jnp.float32, least / len(cuts), top_value / len(cuts))
        loudness = loudness * jnp.repeat(jnp.exp(draws), extent[axis_at] // parts).reshape((-1,) + (1,) * (len(extent) - 1 - axis_at))
    return loudness


def normal_values(key, extent, width, bound, cuts=(), held_as=jnp.bfloat16):
    loudness = block_scale(key, extent, cuts, -0.22, 0.18) if cuts else 1.0
    entries = jax.random.normal(key, extent, jnp.float32) * width * loudness
    return jnp.minimum(jnp.maximum(entries, -bound), bound).astype(held_as)


def setup_inputs(seed: int = 0) -> dict:
    streams_of = jax.random.split(jax.random.key(seed), 35)
    block_in = normal_values(streams_of[0], (TOKENS, D), 1.0, 6.0, ((0, 32),))
    out_grad = normal_values(streams_of[1], (TOKENS, D), 1.0, 6.0, ((0, 32),))
    slot_group = draw_slot_group(jax.random.fold_in(streams_of[34], 71), 0)
    decay_rate = jnp.clip(jnp.exp(jax.random.uniform(streams_of[3], (D,), jnp.float32, math.log(0.3), math.log(12.0))), 0.3, 12.0)
    norm_gain = jnp.clip(1.0 + 0.18 * jax.random.normal(streams_of[4], (2, D), jnp.float32), 0.1, 1.9)
    norm_gain_moment_one = normal_values(streams_of[5], (2, D), (((4 * D * D + 2 * FF * D) * 81) ** -0.5), 0.00018310547, (), jnp.float32)
    norm_gain_moment_two = jnp.clip(jnp.exp(jax.random.uniform(streams_of[6], (2, D), jnp.float32, math.log(1.5894572324981482e-09), math.log(7.947286384535346e-09))), 1.5894572324981482e-09, 7.947286384535346e-09)
    short_kernel = normal_values(streams_of[7], (3, TAPS, D), 0.6, 3.5, (), jnp.float32)
    short_kernel_moment_one = normal_values(streams_of[8], (3, TAPS, D), (((4 * D * D + 2 * FF * D) * 81) ** -0.5), 0.00018310547, (), jnp.float32)
    short_kernel_moment_two = jnp.clip(jnp.exp(jax.random.uniform(streams_of[9], (3, TAPS, D), jnp.float32, math.log(1.5894572324981482e-09), math.log(7.947286384535346e-09))), 1.5894572324981482e-09, 7.947286384535346e-09)
    skip_bias = normal_values(streams_of[10], (D,), 1.0, 6.0, (), jnp.float32)
    skip_bias_moment_one = normal_values(streams_of[11], (D,), (((4 * D * D + 2 * FF * D) * 81) ** -0.5), 0.00018310547, (), jnp.float32)
    skip_bias_moment_two = jnp.clip(jnp.exp(jax.random.uniform(streams_of[12], (D,), jnp.float32, math.log(1.5894572324981482e-09), math.log(7.947286384535346e-09))), 1.5894572324981482e-09, 7.947286384535346e-09)
    filter_first = normal_values(streams_of[13], (EMBED, FILTER), EMBED ** -0.5, 1.0, (), jnp.float32)
    filter_first_moment_one = normal_values(streams_of[14], (EMBED, FILTER), (((4 * D * D + 2 * FF * D) * 81) ** -0.5), 0.00018310547, (), jnp.float32)
    filter_first_moment_two = jnp.clip(jnp.exp(jax.random.uniform(streams_of[15], (EMBED, FILTER), jnp.float32, math.log(1.5894572324981482e-09), math.log(7.947286384535346e-09))), 1.5894572324981482e-09, 7.947286384535346e-09)
    filter_inner = normal_values(streams_of[16], (2, FILTER, FILTER), FILTER ** -0.5, 0.75, (), jnp.float32)
    filter_inner_moment_one = normal_values(streams_of[17], (2, FILTER, FILTER), (((4 * D * D + 2 * FF * D) * 81) ** -0.5), 0.00018310547, (), jnp.float32)
    filter_inner_moment_two = jnp.clip(jnp.exp(jax.random.uniform(streams_of[18], (2, FILTER, FILTER), jnp.float32, math.log(1.5894572324981482e-09), math.log(7.947286384535346e-09))), 1.5894572324981482e-09, 7.947286384535346e-09)
    filter_last = normal_values(streams_of[19], (FILTER, D), (3 * SLOT) ** -0.5, 0.109375, (), jnp.float32)
    filter_last_moment_one = normal_values(streams_of[20], (FILTER, D), (((4 * D * D + 2 * FF * D) * 81) ** -0.5), 0.00018310547, (), jnp.float32)
    filter_last_moment_two = jnp.clip(jnp.exp(jax.random.uniform(streams_of[21], (FILTER, D), jnp.float32, math.log(1.5894572324981482e-09), math.log(7.947286384535346e-09))), 1.5894572324981482e-09, 7.947286384535346e-09)
    in_weight = normal_values(streams_of[22], (3, D, D), D ** -0.5, 0.1875, ((1, 4), (2, 8)), jnp.float32)
    in_weight_moment_one = normal_values(streams_of[23], (3, D, D), (((4 * D * D + 2 * FF * D) * 81) ** -0.5), 0.00018310547, ((1, 4), (2, 8)), jnp.float32)
    in_weight_moment_two = jnp.clip(jnp.exp(math.log(7.947286384535346e-09) - 1.609438 * jax.random.uniform(streams_of[24], (3, D, D), jnp.float32) ** block_scale(streams_of[24], (3, D, D), ((1, 4), (2, 8)), -0.2, 0.2)), 1.5894572324981482e-09, 7.947286384535346e-09)
    out_weight = normal_values(streams_of[25], (D, D), D ** -0.5, 0.1875, ((0, 4), (1, 8)), jnp.float32)
    out_weight_moment_one = normal_values(streams_of[26], (D, D), (((4 * D * D + 2 * FF * D) * 81) ** -0.5), 0.00018310547, ((0, 4), (1, 8)), jnp.float32)
    out_weight_moment_two = jnp.clip(jnp.exp(math.log(7.947286384535346e-09) - 1.609438 * jax.random.uniform(streams_of[27], (D, D), jnp.float32) ** block_scale(streams_of[27], (D, D), ((0, 4), (1, 8)), -0.2, 0.2)), 1.5894572324981482e-09, 7.947286384535346e-09)
    up_weight = normal_values(streams_of[28], (FF, D), D ** -0.5, 0.1875, ((0, 4), (1, 8)), jnp.float32)
    up_weight_moment_one = normal_values(streams_of[29], (FF, D), (((4 * D * D + 2 * FF * D) * 81) ** -0.5), 0.00018310547, ((0, 4), (1, 8)), jnp.float32)
    up_weight_moment_two = jnp.clip(jnp.exp(math.log(7.947286384535346e-09) - 1.609438 * jax.random.uniform(streams_of[30], (FF, D), jnp.float32) ** block_scale(streams_of[30], (FF, D), ((0, 4), (1, 8)), -0.2, 0.2)), 1.5894572324981482e-09, 7.947286384535346e-09)
    down_weight = normal_values(streams_of[31], (FF, D), FF ** -0.5, 0.09375, ((0, 4), (1, 8)), jnp.float32)
    down_weight_moment_one = normal_values(streams_of[32], (FF, D), (((4 * D * D + 2 * FF * D) * 81) ** -0.5), 0.00018310547, ((0, 4), (1, 8)), jnp.float32)
    down_weight_moment_two = jnp.clip(jnp.exp(math.log(7.947286384535346e-09) - 1.609438 * jax.random.uniform(streams_of[33], (FF, D), jnp.float32) ** block_scale(streams_of[33], (FF, D), ((0, 4), (1, 8)), -0.2, 0.2)), 1.5894572324981482e-09, 7.947286384535346e-09)
    return dict(block_in=block_in, out_grad=out_grad, slot_group=slot_group, decay_rate=decay_rate, norm_gain=norm_gain, norm_gain_moment_one=norm_gain_moment_one, norm_gain_moment_two=norm_gain_moment_two, short_kernel=short_kernel, short_kernel_moment_one=short_kernel_moment_one, short_kernel_moment_two=short_kernel_moment_two, skip_bias=skip_bias, skip_bias_moment_one=skip_bias_moment_one, skip_bias_moment_two=skip_bias_moment_two, filter_first=filter_first, filter_first_moment_one=filter_first_moment_one, filter_first_moment_two=filter_first_moment_two, filter_inner=filter_inner, filter_inner_moment_one=filter_inner_moment_one, filter_inner_moment_two=filter_inner_moment_two, filter_last=filter_last, filter_last_moment_one=filter_last_moment_one, filter_last_moment_two=filter_last_moment_two, in_weight=in_weight, in_weight_moment_one=in_weight_moment_one, in_weight_moment_two=in_weight_moment_two, out_weight=out_weight, out_weight_moment_one=out_weight_moment_one, out_weight_moment_two=out_weight_moment_two, up_weight=up_weight, up_weight_moment_one=up_weight_moment_one, up_weight_moment_two=up_weight_moment_two, down_weight=down_weight, down_weight_moment_one=down_weight_moment_one, down_weight_moment_two=down_weight_moment_two)


EPSILON = 1e-05
HIGHEST = lax.Precision.HIGHEST
BETA_ONE = 0.9
BETA_TWO = 0.95
LEARN_RATE = 0.01
WEIGHT_DECAY = 0.1
ADAM_EPSILON = 1e-08
CLIP_NORM = 1.0

@jax.custom_vjp
def low(v):
    return lax.optimization_barrier(v.astype(jnp.bfloat16)).astype(jnp.float32)

@jax.custom_vjp
def low_back(v):
    return v

def low_keep(v):
    return (low(v), None)

def low_pass(kept, grad):
    return (grad,)

def back_keep(v):
    return (v, None)

def back_low(kept, grad):
    return (low(grad),)
low.defvjp(low_keep, low_pass)
low_back.defvjp(back_keep, back_low)

def layer_norm(values, gain_row):
    mean_val = lax.optimization_barrier(jnp.mean(values, axis=-1, keepdims=True))
    centered = values - mean_val
    variance = lax.optimization_barrier(jnp.mean(centered * centered, axis=-1, keepdims=True))
    return centered * lax.rsqrt(variance + EPSILON) * gain_row

def filter_taps(length, first_layer, inner_layers, last_layer, decay_row):
    position = jnp.arange(length).astype(jnp.float32)
    frequency = jnp.linspace(0.0001, 15.0, 16).astype(jnp.float32)
    angles = 2.0 * math.pi / length * position[:, None] * frequency[None, :]
    embedded = jnp.concatenate([position[:, None] / (length - 1), jnp.cos(angles), -jnp.sin(angles)], axis=1)
    hidden = jnp.sin(jnp.dot(embedded, first_layer, precision=HIGHEST, preferred_element_type=jnp.float32))
    hidden = jnp.sin(jnp.dot(hidden, inner_layers[0], precision=HIGHEST, preferred_element_type=jnp.float32))
    hidden = jnp.sin(jnp.dot(hidden, inner_layers[1], precision=HIGHEST, preferred_element_type=jnp.float32))
    raw_taps = jnp.dot(hidden, last_layer, precision=HIGHEST, preferred_element_type=jnp.float32)
    return raw_taps * jnp.exp(-decay_row[None, :] * position[:, None] / (length - 1))

def fft_conv(signal, filter_rows):
    length = signal.shape[-2]
    padded_len = 2 * length
    spectrum = jnp.fft.rfft(signal, n=padded_len, axis=-2) * jnp.fft.rfft(filter_rows, n=padded_len, axis=-2)
    return jnp.fft.irfft(spectrum, n=padded_len, axis=-2)[..., :length, :]

def forward(params, slot_inputs, slot_group, decay_rate):
    gain_rows, kernel, skip_row, first_layer, inner_layers, last_layer, in_full, out_full, up_full, down_full = params
    long_taps = filter_taps(SLOT, first_layer, inner_layers, last_layer, decay_rate)
    short_taps = filter_taps(SHORT, first_layer, inner_layers, last_layer, decay_rate)
    in_low = low(in_full)
    out_low = low(out_full)
    up_low = low(up_full)
    down_low = low(down_full)

    def one_slot(slot_rows, group_flag):
        normed_in = low(layer_norm(slot_rows, gain_rows[0]))
        projected = low_back(jnp.einsum('td,kcd->tkc', normed_in, in_low, precision=HIGHEST, preferred_element_type=jnp.float32))
        position = jnp.arange(SLOT, dtype=jnp.int32)
        in_seq = jnp.where(group_flag == 0, position, position % SHORT)
        zeros_row = jnp.zeros((1, 3, D), jnp.float32)
        shift_one = jnp.concatenate([zeros_row, projected[:-1]], 0) * (in_seq >= 1).astype(jnp.float32)[:, None, None]
        shift_two = jnp.concatenate([zeros_row, zeros_row, projected[:-2]], 0) * (in_seq >= 2).astype(jnp.float32)[:, None, None]
        conved = kernel[:, 0] * projected + kernel[:, 1] * shift_one + kernel[:, 2] * shift_two
        outer_gate = conved[:, 0]
        gated = conved[:, 2] * conved[:, 1]
        whole_conv = fft_conv(gated, long_taps)
        pieces = fft_conv(gated.reshape(SLOT // SHORT, SHORT, D), short_taps[None]).reshape(SLOT, D)
        mixed_sum = jnp.where(group_flag == 0, whole_conv, pieces) + skip_row * gated
        mixer_y = low(mixed_sum * outer_gate)
        branch = low_back(jnp.dot(mixer_y, out_low, precision=HIGHEST, preferred_element_type=jnp.float32))
        hidden_in = slot_rows + branch
        normed_mid = low(layer_norm(hidden_in, gain_rows[1]))
        pre_act = low_back(jnp.dot(normed_mid, up_low.T, precision=HIGHEST, preferred_element_type=jnp.float32))
        activated = low(jax.nn.gelu(pre_act))
        return hidden_in + jnp.dot(activated, down_low, precision=HIGHEST, preferred_element_type=jnp.float32)
    slot_step = jax.checkpoint(one_slot)

    def scan_body(carried, scan_item):
        return (carried, slot_step(scan_item[0], scan_item[1]))
    unused, slot_outs = lax.scan(scan_body, jnp.zeros((), jnp.float32), (slot_inputs, slot_group))
    return slot_outs

def adam_update(weight, moment_one, moment_two, gradient, clip_scale, decayed):
    clipped = gradient * clip_scale
    new_one = BETA_ONE * moment_one + (1.0 - BETA_ONE) * clipped
    new_two = BETA_TWO * moment_two + (1.0 - BETA_TWO) * clipped * clipped
    change = new_one / (1.0 - BETA_ONE ** STEP) / (jnp.sqrt(new_two / (1.0 - BETA_TWO ** STEP)) + ADAM_EPSILON)
    if decayed:
        change = change + WEIGHT_DECAY * weight
    return (-LEARN_RATE * change, new_one, new_two)

def reference(block_in, out_grad, slot_group, decay_rate, norm_gain, norm_gain_moment_one, norm_gain_moment_two, short_kernel, short_kernel_moment_one, short_kernel_moment_two, skip_bias, skip_bias_moment_one, skip_bias_moment_two, filter_first, filter_first_moment_one, filter_first_moment_two, filter_inner, filter_inner_moment_one, filter_inner_moment_two, filter_last, filter_last_moment_one, filter_last_moment_two, in_weight, in_weight_moment_one, in_weight_moment_two, out_weight, out_weight_moment_one, out_weight_moment_two, up_weight, up_weight_moment_one, up_weight_moment_two, down_weight, down_weight_moment_one, down_weight_moment_two):
    params = (norm_gain, short_kernel, skip_bias, filter_first, filter_inner, filter_last, in_weight, out_weight, up_weight, down_weight)
    slot_inputs = block_in.astype(jnp.float32).reshape(N_DP, SLOT, D)

    def wrapped(param_tuple, inputs_all):
        return forward(param_tuple, inputs_all, slot_group, decay_rate)
    slot_outs, back_fn = jax.vjp(wrapped, params, slot_inputs)
    gradients, input_grads = back_fn(out_grad.astype(jnp.float32).reshape(N_DP, SLOT, D))
    square_total = jnp.zeros((), jnp.float32)
    for gradient in gradients:
        square_total = square_total + jnp.sum(gradient * gradient)
    grad_norm = jnp.sqrt(square_total)
    clip_scale = jnp.minimum(1.0, CLIP_NORM / (grad_norm + 1e-06))
    firsts = (norm_gain_moment_one, short_kernel_moment_one, skip_bias_moment_one, filter_first_moment_one, filter_inner_moment_one, filter_last_moment_one, in_weight_moment_one, out_weight_moment_one, up_weight_moment_one, down_weight_moment_one)
    seconds = (norm_gain_moment_two, short_kernel_moment_two, skip_bias_moment_two, filter_first_moment_two, filter_inner_moment_two, filter_last_moment_two, in_weight_moment_two, out_weight_moment_two, up_weight_moment_two, down_weight_moment_two)
    decayed_flags = (False, False, False, True, True, True, True, True, True, True)
    updates = [adam_update(params[index], firsts[index], seconds[index], gradients[index], clip_scale, decayed_flags[index]) for index in range(10)]
    norm_gain_update, new_norm_gain_moment_one, new_norm_gain_moment_two = updates[0]
    short_kernel_update, new_short_kernel_moment_one, new_short_kernel_moment_two = updates[1]
    skip_bias_update, new_skip_bias_moment_one, new_skip_bias_moment_two = updates[2]
    filter_first_update, new_filter_first_moment_one, new_filter_first_moment_two = updates[3]
    filter_inner_update, new_filter_inner_moment_one, new_filter_inner_moment_two = updates[4]
    filter_last_update, new_filter_last_moment_one, new_filter_last_moment_two = updates[5]
    in_weight_update, new_in_weight_moment_one, new_in_weight_moment_two = updates[6]
    out_weight_update, new_out_weight_moment_one, new_out_weight_moment_two = updates[7]
    up_weight_update, new_up_weight_moment_one, new_up_weight_moment_two = updates[8]
    down_weight_update, new_down_weight_moment_one, new_down_weight_moment_two = updates[9]
    block_out = slot_outs.reshape(TOKENS, D).astype(jnp.bfloat16)
    in_grad = input_grads.reshape(TOKENS, D)
    return (block_out, in_grad, grad_norm, norm_gain_update, new_norm_gain_moment_one, new_norm_gain_moment_two, short_kernel_update, new_short_kernel_moment_one, new_short_kernel_moment_two, skip_bias_update, new_skip_bias_moment_one, new_skip_bias_moment_two, filter_first_update, new_filter_first_moment_one, new_filter_first_moment_two, filter_inner_update, new_filter_inner_moment_one, new_filter_inner_moment_two, filter_last_update, new_filter_last_moment_one, new_filter_last_moment_two, in_weight_update, new_in_weight_moment_one, new_in_weight_moment_two, out_weight_update, new_out_weight_moment_one, new_out_weight_moment_two, up_weight_update, new_up_weight_moment_one, new_up_weight_moment_two, down_weight_update, new_down_weight_moment_one, new_down_weight_moment_two)
```

```python
import functools
import math

import jax
import jax.numpy as jnp
from jax import lax
from jax.experimental import pallas as pl
from jax.experimental.pallas import tpu as pltpu
from jax.sharding import PartitionSpec as P

SHORT = 256
STEP = 10
EPSILON = 1e-05
HIGHEST = lax.Precision.HIGHEST
HIGH = lax.Precision.HIGH
BETA_ONE = 0.9
BETA_TWO = 0.95
LEARN_RATE = 0.01
WEIGHT_DECAY = 0.1
ADAM_EPSILON = 1e-08
CLIP_NORM = 1.0
EDGE = 16
LANES = 128
BF = jnp.bfloat16
F32 = jnp.float32
ROWS_ROWS = (((1,), (1,)), ((), ()))
COLS_COLS = (((0,), (0,)), ((), ()))
MESH_IDS = pl.DeviceIdType.MESH


def norm_parts(values):
    mean_val = jnp.mean(values, axis=-1, keepdims=True)
    centered = values - mean_val
    variance = jnp.mean(centered * centered, axis=-1, keepdims=True)
    scale = lax.rsqrt(variance + EPSILON)
    return centered * scale, scale


def norm_back(grad, xhat, scale, gain_row):
    e = grad * gain_row
    mean_e = jnp.mean(e, axis=-1, keepdims=True)
    mean_ex = jnp.mean(e * xhat, axis=-1, keepdims=True)
    return scale * (e - mean_e - xhat * mean_ex), jnp.sum(grad * xhat, axis=0)


def transform_tables(slot, seq_len, tok):
    in_seq = tok % seq_len
    block = tok // seq_len
    inner = 32
    outer = slot // inner
    step = math.pi / (2.0 * seq_len.astype(F32))

    def table(odd):
        turns = (odd[:, None] * in_seq[None, :]) % (4 * seq_len)
        angle = turns.astype(F32) * step
        return jnp.cos(angle), jnp.sin(angle)

    index_a = jnp.arange(outer, dtype=jnp.int32) * inner
    cos_a, sin_a = table(2 * (index_a % seq_len))
    same = (index_a // seq_len)[:, None] == block[None, :]
    cos_a = jnp.where(same, cos_a, 0.0)
    sin_a = jnp.where(same, sin_a, 0.0)
    cos_b, sin_b = table(2 * jnp.arange(inner, dtype=jnp.int32) + 1)
    cos_a, sin_a, cos_b, sin_b = lax.optimization_barrier((cos_a, sin_a, cos_b, sin_b))
    cos_all = cos_a[:, None] * cos_b[None] - sin_a[:, None] * sin_b[None]
    sin_all = sin_a[:, None] * cos_b[None] + cos_a[:, None] * sin_b[None]
    return jnp.concatenate(
        [cos_all.reshape(slot, slot), sin_all.reshape(slot, slot)], axis=0
    )


def embed(seq_len, tok):
    position = (tok % seq_len).astype(F32)
    length = seq_len.astype(F32)
    frequency = jnp.linspace(0.0001, 15.0, 16).astype(F32)
    angles = 2.0 * math.pi / length * position[:, None] * frequency[None, :]
    place = position[:, None] / (length - 1.0)
    return jnp.concatenate([place, jnp.cos(angles), -jnp.sin(angles)], axis=1), place


def filter_taps(embedded, decay, first_layer, inner_layers, last_layer):
    def dense(a, b):
        return jnp.dot(a, b, precision=HIGHEST, preferred_element_type=F32)

    hidden = jnp.sin(dense(embedded, first_layer))
    hidden = jnp.sin(dense(hidden, inner_layers[0]))
    hidden = jnp.sin(dense(hidden, inner_layers[1]))
    return dense(hidden, last_layer) * decay


def adam_update(weight, moment_one, moment_two, gradient, clip_scale, decayed):
    clipped = gradient * clip_scale
    new_one = BETA_ONE * moment_one + (1.0 - BETA_ONE) * clipped
    new_two = BETA_TWO * moment_two + (1.0 - BETA_TWO) * clipped * clipped
    change = (
        new_one
        / (1.0 - BETA_ONE**STEP)
        / (jnp.sqrt(new_two / (1.0 - BETA_TWO**STEP)) + ADAM_EPSILON)
    )
    if decayed:
        change = change + WEIGHT_DECAY * weight
    return (-LEARN_RATE * change, new_one, new_two)


def per_device(
    paths,
    block_in,
    out_grad,
    slot_group,
    decay_rate,
    *state,
):
    names = (
        "norm_gain",
        "short_kernel",
        "skip_bias",
        "filter_first",
        "filter_inner",
        "filter_last",
        "in_weight",
        "out_weight",
        "up_weight",
        "down_weight",
    )
    params = dict(zip(names, state[0::3]))
    firsts = dict(zip(names, state[1::3]))
    seconds = dict(zip(names, state[2::3]))
    norm_gain, short_kernel, skip_bias = (params[n] for n in names[:3])
    filter_first, filter_inner, filter_last = (params[n] for n in names[3:6])

    n_mp = lax.axis_size("mp")
    rows, width = block_in.shape
    slot = rows * n_mp
    wide = 3 * width
    channels = width // n_mp
    mp_at = lax.axis_index("mp")
    start_chan = mp_at * channels
    seq_len = jnp.where(slot_group[0] == 0, slot, SHORT).astype(jnp.int32)
    forward_ring = [(i, i + 1) for i in range(n_mp - 1)]
    backward_ring = [(i + 1, i) for i in range(n_mp - 1)]

    big = [params[n].astype(BF) for n in names[6:]]
    in_full, out_full = paths.gather_mixer(big[0], big[1])
    up_full, down_full = paths.gather_ffn(big[2], big[3])

    edge_in = lax.ppermute(block_in[-EDGE:], "mp", forward_ring)
    tok_ext = jnp.concatenate([edge_in, block_in], axis=0).astype(F32)
    xhat_ext, scale_ext = norm_parts(tok_ext)
    normed_ext = (xhat_ext * norm_gain[0]).astype(BF)
    residual, xhat_one, scale_one = tok_ext[EDGE:], xhat_ext[EDGE:], scale_ext[EDGE:]
    normed_one = normed_ext[EDGE:]
    proj_ext = lax.dot_general(
        normed_ext, in_full.reshape(wide, width), ROWS_ROWS, preferred_element_type=F32
    )
    tok = mp_at * rows + jnp.arange(rows, dtype=jnp.int32)
    pos = tok % seq_len
    kern = [short_kernel[:, j].reshape(1, wide) for j in range(3)]
    shifted = [proj_ext[EDGE:]] + [
        jnp.where((pos >= j)[:, None], proj_ext[EDGE - j : -j], 0.0) for j in (1, 2)
    ]
    conved = kern[0] * shifted[0] + kern[1] * shifted[1] + kern[2] * shifted[2]
    outer, gate, value = (conved[:, k * width : (k + 1) * width] for k in range(3))
    gated = value * gate

    slot_tok = jnp.arange(slot, dtype=jnp.int32)
    table = transform_tables(slot, seq_len, slot_tok)
    embedded, place = embed(seq_len, slot_tok)
    decay_local = lax.dynamic_slice_in_dim(decay_rate, start_chan, channels, 0)
    last_local = lax.dynamic_slice_in_dim(filter_last, start_chan, channels, 1)
    decay = jnp.exp(-decay_local[None, :] * place)
    taps, taps_back = jax.vjp(
        functools.partial(filter_taps, embedded, decay),
        filter_first,
        filter_inner,
        last_local,
    )
    norm_of = 1.0 / seq_len.astype(F32)

    def spectrum(signal):
        both = jnp.dot(table, signal, precision=HIGH, preferred_element_type=F32)
        return both[:slot], both[slot:]

    def signal_of(cos_part, sin_part):
        both = jnp.concatenate([cos_part, sin_part], axis=0)
        return norm_of * lax.dot_general(
            table, both, COLS_COLS, precision=HIGH, preferred_element_type=F32
        )

    def to_channels(values):
        return lax.all_to_all(
            values.astype(BF), "mp", split_axis=1, concat_axis=0, tiled=True
        ).astype(F32)

    def to_tokens(values):
        return lax.all_to_all(
            values.astype(BF), "mp", split_axis=0, concat_axis=1, tiled=True
        ).astype(F32)

    taps_cos, taps_sin = spectrum(taps)
    gated_cos, gated_sin = spectrum(to_channels(gated))
    conv_sum = to_tokens(
        signal_of(
            gated_cos * taps_cos - gated_sin * taps_sin,
            gated_cos * taps_sin + gated_sin * taps_cos,
        )
    )
    mixed = conv_sum + skip_bias * gated
    mixer_low = (mixed * outer).astype(BF)
    hidden_in = residual + jnp.dot(mixer_low, out_full, preferred_element_type=F32)

    xhat_two, scale_two = norm_parts(hidden_in)
    normed_two = (xhat_two * norm_gain[1]).astype(BF)
    pre_act = lax.dot_general(normed_two, up_full, ROWS_ROWS, preferred_element_type=F32)
    activated, gelu_back = jax.vjp(jax.nn.gelu, pre_act)
    activ_low = activated.astype(BF)
    block_out = (
        hidden_in + jnp.dot(activ_low, down_full, preferred_element_type=F32)
    ).astype(BF)
    act_grad = lax.dot_general(out_grad, down_full, ROWS_ROWS, preferred_element_type=F32)
    pre_grad = gelu_back(act_grad)[0].astype(BF)
    ffn_sums = paths.reduce_ffn(
        (pre_grad, normed_two, None), (activ_low, out_grad, None)
    )
    mid_grad = jnp.dot(pre_grad, up_full, preferred_element_type=F32)
    hidden_part, gain_two_grad = norm_back(mid_grad, xhat_two, scale_two, norm_gain[1])
    hidden_grad = out_grad.astype(F32) + hidden_part
    hidden_low = hidden_grad.astype(BF)

    y_grad = lax.dot_general(hidden_low, out_full, ROWS_ROWS, preferred_element_type=F32)
    q_grad = y_grad * outer
    outer_grad = mixed * y_grad
    q_cos, q_sin = spectrum(to_channels(q_grad))
    gated_grad = (
        to_tokens(
            signal_of(
                q_cos * taps_cos + q_sin * taps_sin, q_sin * taps_cos - q_cos * taps_sin
            )
        )
        + skip_bias * q_grad
    )
    taps_grad = signal_of(
        q_cos * gated_cos + q_sin * gated_sin, q_sin * gated_cos - q_cos * gated_sin
    )
    first_grad, inner_grad, last_grad = taps_back(taps_grad)
    skip_grad = jnp.sum(q_grad * gated, axis=0)
    conv_grad = jnp.concatenate(
        [outer_grad, gated_grad * value, gated_grad * gate], axis=1
    )
    edge_grad = lax.ppermute(conv_grad[:8], "mp", backward_ring)
    grad_ext = jnp.concatenate([conv_grad, edge_grad], axis=0)
    pos_ext = (mp_at * rows + jnp.arange(rows + 8, dtype=jnp.int32)) % seq_len
    proj_grad = kern[0] * conv_grad
    for j in (1, 2):
        proj_grad = proj_grad + kern[j] * jnp.where(
            (pos_ext[j : rows + j] >= j)[:, None], grad_ext[j : rows + j], 0.0
        )
    proj_low = proj_grad.astype(BF)
    kern_grad = jnp.stack(
        [jnp.sum(conv_grad * shifted[j], axis=0) for j in range(3)]
    )
    kern_grad = kern_grad.reshape(3, 3, width).transpose(1, 0, 2)
    normed_grad = jnp.dot(
        proj_low, in_full.reshape(wide, width), preferred_element_type=F32
    )
    resid_part, gain_one_grad = norm_back(normed_grad, xhat_one, scale_one, norm_gain[0])
    in_grad = hidden_grad + resid_part

    last_full = lax.dynamic_update_slice_in_dim(
        jnp.zeros_like(filter_last), last_grad, start_chan, 1
    )
    small = (
        jnp.stack([gain_one_grad, gain_two_grad]),
        kern_grad,
        skip_grad,
        first_grad,
        inner_grad,
        last_full,
    )
    gradients, square_total = paths.reduce_mixer(
        (proj_low, normed_one, 3), (mixer_low, hidden_low, None), small, ffn_sums
    )
    grad_norm = jnp.sqrt(square_total)
    clip_scale = jnp.minimum(1.0, CLIP_NORM / (grad_norm + 1e-06))
    outputs = [block_out, in_grad, grad_norm]
    for index, name in enumerate(names):
        outputs.extend(
            adam_update(
                params[name],
                firsts[name],
                seconds[name],
                gradients[index],
                clip_scale,
                index >= 3,
            )
        )
    return tuple(outputs)


def squares(values):
    return sum(jnp.sum(v * v) for v in values)


class PlainPaths:
    def gather(self, shard):
        along = shard.ndim - 1
        part = lax.all_gather(shard, "dp", axis=along, tiled=True)
        return lax.all_gather(part, "mp", axis=along - 1, tiled=True)

    def gather_mixer(self, in_shard, out_shard):
        return self.gather(in_shard), self.gather(out_shard)

    def gather_ffn(self, up_shard, down_shard):
        return self.gather(up_shard), self.gather(down_shard)

    def reduced(self, left, right, parts):
        grad = lax.dot_general(left, right, COLS_COLS, preferred_element_type=F32)
        if parts:
            grad = grad.reshape(parts, -1, grad.shape[-1])
        along = grad.ndim - 1
        part = lax.psum_scatter(grad, "mp", scatter_dimension=along - 1, tiled=True)
        return lax.psum_scatter(part, "dp", scatter_dimension=along, tiled=True)

    def reduce_ffn(self, up_pair, down_pair):
        return self.reduced(*up_pair), self.reduced(*down_pair)

    def reduce_mixer(self, in_pair, out_pair, small, ffn_sums):
        large = (self.reduced(*in_pair), self.reduced(*out_pair)) + tuple(ffn_sums)
        small = lax.psum(small, ("dp", "mp"))
        total = lax.psum(squares(large), ("dp", "mp")) + squares(small)
        return tuple(small) + large, total


def choose_paths(mesh):
    return PlainPaths()


def solution(mesh):
    tokens = P(("dp", "mp"), None)
    weights = (P(None, "mp", "dp"),) * 3 + (P("mp", "dp"),) * 9
    return jax.shard_map(
        functools.partial(per_device, choose_paths(mesh)),
        mesh=mesh,
        in_specs=(tokens, tokens, P("dp"), P()) + (P(),) * 18 + weights,
        out_specs=(tokens, tokens, P()) + (P(),) * 18 + weights,
        check_vma=False,
    )
```

```python
import functools
import math

import jax
import jax.numpy as jnp
from jax import lax
from jax.experimental import pallas as pl
from jax.experimental.pallas import tpu as pltpu
from jax.sharding import PartitionSpec as P

SHORT = 256
STEP = 10
EPSILON = 1e-05
HIGHEST = lax.Precision.HIGHEST
HIGH = lax.Precision.HIGH
BETA_ONE = 0.9
BETA_TWO = 0.95
LEARN_RATE = 0.01
WEIGHT_DECAY = 0.1
ADAM_EPSILON = 1e-08
CLIP_NORM = 1.0
EDGE = 16
LANES = 128
BF = jnp.bfloat16
F32 = jnp.float32
ROWS_ROWS = (((1,), (1,)), ((), ()))
COLS_COLS = (((0,), (0,)), ((), ()))
MESH_IDS = pl.DeviceIdType.MESH


def norm_parts(values):
    mean_val = jnp.mean(values, axis=-1, keepdims=True)
    centered = values - mean_val
    variance = jnp.mean(centered * centered, axis=-1, keepdims=True)
    scale = lax.rsqrt(variance + EPSILON)
    return centered * scale, scale


def norm_back(grad, xhat, scale, gain_row):
    e = grad * gain_row
    mean_e = jnp.mean(e, axis=-1, keepdims=True)
    mean_ex = jnp.mean(e * xhat, axis=-1, keepdims=True)
    return scale * (e - mean_e - xhat * mean_ex), jnp.sum(grad * xhat, axis=0)


def transform_tables(slot, seq_len, tok):
    in_seq = tok % seq_len
    block = tok // seq_len
    inner = 32
    outer = slot // inner
    step = math.pi / (2.0 * seq_len.astype(F32))

    def table(odd):
        turns = (odd[:, None] * in_seq[None, :]) % (4 * seq_len)
        angle = turns.astype(F32) * step
        return jnp.cos(angle), jnp.sin(angle)

    index_a = jnp.arange(outer, dtype=jnp.int32) * inner
    cos_a, sin_a = table(2 * (index_a % seq_len))
    same = (index_a // seq_len)[:, None] == block[None, :]
    cos_a = jnp.where(same, cos_a, 0.0)
    sin_a = jnp.where(same, sin_a, 0.0)
    cos_b, sin_b = table(2 * jnp.arange(inner, dtype=jnp.int32) + 1)
    cos_a, sin_a, cos_b, sin_b = lax.optimization_barrier((cos_a, sin_a, cos_b, sin_b))
    cos_all = cos_a[:, None] * cos_b[None] - sin_a[:, None] * sin_b[None]
    sin_all = sin_a[:, None] * cos_b[None] + cos_a[:, None] * sin_b[None]
    return jnp.concatenate(
        [cos_all.reshape(slot, slot), sin_all.reshape(slot, slot)], axis=0
    )


def embed(seq_len, tok):
    position = (tok % seq_len).astype(F32)
    length = seq_len.astype(F32)
    frequency = jnp.linspace(0.0001, 15.0, 16).astype(F32)
    angles = 2.0 * math.pi / length * position[:, None] * frequency[None, :]
    place = position[:, None] / (length - 1.0)
    return jnp.concatenate([place, jnp.cos(angles), -jnp.sin(angles)], axis=1), place


def filter_taps(embedded, decay, first_layer, inner_layers, last_layer):
    def dense(a, b):
        return jnp.dot(a, b, precision=HIGHEST, preferred_element_type=F32)

    hidden = jnp.sin(dense(embedded, first_layer))
    hidden = jnp.sin(dense(hidden, inner_layers[0]))
    hidden = jnp.sin(dense(hidden, inner_layers[1]))
    return dense(hidden, last_layer) * decay


def adam_update(weight, moment_one, moment_two, gradient, clip_scale, decayed):
    clipped = gradient * clip_scale
    new_one = BETA_ONE * moment_one + (1.0 - BETA_ONE) * clipped
    new_two = BETA_TWO * moment_two + (1.0 - BETA_TWO) * clipped * clipped
    change = (
        new_one
        / (1.0 - BETA_ONE**STEP)
        / (jnp.sqrt(new_two / (1.0 - BETA_TWO**STEP)) + ADAM_EPSILON)
    )
    if decayed:
        change = change + WEIGHT_DECAY * weight
    return (-LEARN_RATE * change, new_one, new_two)


def per_device(
    paths,
    block_in,
    out_grad,
    slot_group,
    decay_rate,
    *state,
):
    names = (
        "norm_gain",
        "short_kernel",
        "skip_bias",
        "filter_first",
        "filter_inner",
        "filter_last",
        "in_weight",
        "out_weight",
        "up_weight",
        "down_weight",
    )
    params = dict(zip(names, state[0::3]))
    firsts = dict(zip(names, state[1::3]))
    seconds = dict(zip(names, state[2::3]))
    norm_gain, short_kernel, skip_bias = (params[n] for n in names[:3])
    filter_first, filter_inner, filter_last = (params[n] for n in names[3:6])

    n_mp = lax.axis_size("mp")
    rows, width = block_in.shape
    slot = rows * n_mp
    wide = 3 * width
    channels = width // n_mp
    mp_at = lax.axis_index("mp")
    start_chan = mp_at * channels
    seq_len = jnp.where(slot_group[0] == 0, slot, SHORT).astype(jnp.int32)
    forward_ring = [(i, i + 1) for i in range(n_mp - 1)]
    backward_ring = [(i + 1, i) for i in range(n_mp - 1)]

    big = [params[n].astype(BF) for n in names[6:]]
    in_full, out_full = paths.gather_mixer(big[0], big[1])
    up_full, down_full = paths.gather_ffn(big[2], big[3])

    edge_in = lax.ppermute(block_in[-EDGE:], "mp", forward_ring)
    tok_ext = jnp.concatenate([edge_in, block_in], axis=0).astype(F32)
    xhat_ext, scale_ext = norm_parts(tok_ext)
    normed_ext = (xhat_ext * norm_gain[0]).astype(BF)
    residual, xhat_one, scale_one = tok_ext[EDGE:], xhat_ext[EDGE:], scale_ext[EDGE:]
    normed_one = normed_ext[EDGE:]
    proj_ext = lax.dot_general(
        normed_ext, in_full.reshape(wide, width), ROWS_ROWS, preferred_element_type=F32
    )
    tok = mp_at * rows + jnp.arange(rows, dtype=jnp.int32)
    pos = tok % seq_len
    kern = [short_kernel[:, j].reshape(1, wide) for j in range(3)]
    shifted = [proj_ext[EDGE:]] + [
        jnp.where((pos >= j)[:, None], proj_ext[EDGE - j : -j], 0.0) for j in (1, 2)
    ]
    conved = kern[0] * shifted[0] + kern[1] * shifted[1] + kern[2] * shifted[2]
    outer, gate, value = (conved[:, k * width : (k + 1) * width] for k in range(3))
    gated = value * gate

    slot_tok = jnp.arange(slot, dtype=jnp.int32)
    table = transform_tables(slot, seq_len, slot_tok)
    embedded, place = embed(seq_len, slot_tok)
    decay_local = lax.dynamic_slice_in_dim(decay_rate, start_chan, channels, 0)
    last_local = lax.dynamic_slice_in_dim(filter_last, start_chan, channels, 1)
    decay = jnp.exp(-decay_local[None, :] * place)
    taps, taps_back = jax.vjp(
        functools.partial(filter_taps, embedded, decay),
        filter_first,
        filter_inner,
        last_local,
    )
    norm_of = 1.0 / seq_len.astype(F32)

    def spectrum(signal):
        both = jnp.dot(table, signal, precision=HIGH, preferred_element_type=F32)
        return both[:slot], both[slot:]

    def signal_of(cos_part, sin_part):
        both = jnp.concatenate([cos_part, sin_part], axis=0)
        return norm_of * lax.dot_general(
            table, both, COLS_COLS, precision=HIGH, preferred_element_type=F32
        )

    def to_channels(values):
        return lax.all_to_all(
            values.astype(BF), "mp", split_axis=1, concat_axis=0, tiled=True
        ).astype(F32)

    def to_tokens(values):
        return lax.all_to_all(
            values.astype(BF), "mp", split_axis=0, concat_axis=1, tiled=True
        ).astype(F32)

    taps_cos, taps_sin = spectrum(taps)
    gated_cos, gated_sin = spectrum(to_channels(gated))
    conv_sum = to_tokens(
        signal_of(
            gated_cos * taps_cos - gated_sin * taps_sin,
            gated_cos * taps_sin + gated_sin * taps_cos,
        )
    )
    mixed = conv_sum + skip_bias * gated
    mixer_low = (mixed * outer).astype(BF)
    hidden_in = residual + jnp.dot(mixer_low, out_full, preferred_element_type=F32)

    xhat_two, scale_two = norm_parts(hidden_in)
    normed_two = (xhat_two * norm_gain[1]).astype(BF)
    pre_act = lax.dot_general(normed_two, up_full, ROWS_ROWS, preferred_element_type=F32)
    activated, gelu_back = jax.vjp(jax.nn.gelu, pre_act)
    activ_low = activated.astype(BF)
    block_out = (
        hidden_in + jnp.dot(activ_low, down_full, preferred_element_type=F32)
    ).astype(BF)
    act_grad = lax.dot_general(out_grad, down_full, ROWS_ROWS, preferred_element_type=F32)
    pre_grad = gelu_back(act_grad)[0].astype(BF)
    ffn_sums = paths.reduce_ffn(
        (pre_grad, normed_two, None), (activ_low, out_grad, None)
    )
    mid_grad = jnp.dot(pre_grad, up_full, preferred_element_type=F32)
    hidden_part, gain_two_grad = norm_back(mid_grad, xhat_two, scale_two, norm_gain[1])
    hidden_grad = out_grad.astype(F32) + hidden_part
    hidden_low = hidden_grad.astype(BF)

    y_grad = lax.dot_general(hidden_low, out_full, ROWS_ROWS, preferred_element_type=F32)
    q_grad = y_grad * outer
    outer_grad = mixed * y_grad
    q_cos, q_sin = spectrum(to_channels(q_grad))
    gated_grad = (
        to_tokens(
            signal_of(
                q_cos * taps_cos + q_sin * taps_sin, q_sin * taps_cos - q_cos * taps_sin
            )
        )
        + skip_bias * q_grad
    )
    taps_grad = signal_of(
        q_cos * gated_cos + q_sin * gated_sin, q_sin * gated_cos - q_cos * gated_sin
    )
    first_grad, inner_grad, last_grad = taps_back(taps_grad)
    skip_grad = jnp.sum(q_grad * gated, axis=0)
    conv_grad = jnp.concatenate(
        [outer_grad, gated_grad * value, gated_grad * gate], axis=1
    )
    edge_grad = lax.ppermute(conv_grad[:8], "mp", backward_ring)
    grad_ext = jnp.concatenate([conv_grad, edge_grad], axis=0)
    pos_ext = (mp_at * rows + jnp.arange(rows + 8, dtype=jnp.int32)) % seq_len
    proj_grad = kern[0] * conv_grad
    for j in (1, 2):
        proj_grad = proj_grad + kern[j] * jnp.where(
            (pos_ext[j : rows + j] >= j)[:, None], grad_ext[j : rows + j], 0.0
        )
    proj_low = proj_grad.astype(BF)
    kern_grad = jnp.stack(
        [jnp.sum(conv_grad * shifted[j], axis=0) for j in range(3)]
    )
    kern_grad = kern_grad.reshape(3, 3, width).transpose(1, 0, 2)
    normed_grad = jnp.dot(
        proj_low, in_full.reshape(wide, width), preferred_element_type=F32
    )
    resid_part, gain_one_grad = norm_back(normed_grad, xhat_one, scale_one, norm_gain[0])
    in_grad = hidden_grad + resid_part

    last_full = lax.dynamic_update_slice_in_dim(
        jnp.zeros_like(filter_last), last_grad, start_chan, 1
    )
    small = (
        jnp.stack([gain_one_grad, gain_two_grad]),
        kern_grad,
        skip_grad,
        first_grad,
        inner_grad,
        last_full,
    )
    gradients, square_total = paths.reduce_mixer(
        (proj_low, normed_one, 3), (mixer_low, hidden_low, None), small, ffn_sums
    )
    grad_norm = jnp.sqrt(square_total)
    clip_scale = jnp.minimum(1.0, CLIP_NORM / (grad_norm + 1e-06))
    outputs = [block_out, in_grad, grad_norm]
    for index, name in enumerate(names):
        outputs.extend(
            adam_update(
                params[name],
                firsts[name],
                seconds[name],
                gradients[index],
                clip_scale,
                index >= 3,
            )
        )
    return tuple(outputs)


def squares(values):
    return sum(jnp.sum(v * v) for v in values)


class PlainPaths:
    def gather(self, shard):
        along = shard.ndim - 1
        part = lax.all_gather(shard, "dp", axis=along, tiled=True)
        return lax.all_gather(part, "mp", axis=along - 1, tiled=True)

    def gather_mixer(self, in_shard, out_shard):
        return self.gather(in_shard), self.gather(out_shard)

    def gather_ffn(self, up_shard, down_shard):
        return self.gather(up_shard), self.gather(down_shard)

    def reduced(self, left, right, parts):
        grad = lax.dot_general(left, right, COLS_COLS, preferred_element_type=F32)
        if parts:
            grad = grad.reshape(parts, -1, grad.shape[-1])
        along = grad.ndim - 1
        part = lax.psum_scatter(grad, "mp", scatter_dimension=along - 1, tiled=True)
        return lax.psum_scatter(part, "dp", scatter_dimension=along, tiled=True)

    def reduce_ffn(self, up_pair, down_pair):
        return self.reduced(*up_pair), self.reduced(*down_pair)

    def reduce_mixer(self, in_pair, out_pair, small, ffn_sums):
        large = (self.reduced(*in_pair), self.reduced(*out_pair)) + tuple(ffn_sums)
        small = lax.psum(small, ("dp", "mp"))
        total = lax.psum(squares(large), ("dp", "mp")) + squares(small)
        return tuple(small) + large, total


class Place:
    def __init__(self, n_mp):
        dp = lax.axis_index("dp")
        self.n_mp = n_mp
        self.dp = dp
        self.z = lax.axis_index("mp")
        self.y, self.x, self.c = dp // 4, (dp // 2) % 2, dp % 2
        self.by_x = (dp + 2 - 4 * self.x, self.z)
        self.by_y = (dp + 4 - 8 * self.y, self.z)
        self.by_core = (dp + 1 - 2 * self.c, self.z)

    def up(self, off):
        return lax.rem(self.z + off, self.n_mp)

    def by_z(self, off):
        return (self.dp, self.up(off))

    def column(self, y, x, c):
        return pl.ds(pl.multiple_of((4 * y + 2 * x + c) * LANES, LANES), LANES)


def greet(here):
    barrier = pltpu.get_barrier_semaphore()
    peers = [here.by_x, here.by_y, here.by_core]
    peers += [here.by_z(off) for off in range(1, here.n_mp)]
    for peer in peers:
        pl.semaphore_signal(barrier, inc=1, device_id=peer, device_id_type=MESH_IDS)
    pl.semaphore_wait(barrier, len(peers))


def push(source, target, sems, index, peer):
    copy = pltpu.make_async_remote_copy(
        src_ref=source,
        dst_ref=target,
        send_sem=sems[0].at[index],
        recv_sem=sems[1].at[index],
        device_id=peer,
        device_id_type=MESH_IDS,
    )
    copy.start()
    return copy


GATHER_COPIES = 39


def gather_kernel(n_mp, count, *refs):
    shards, wholes = refs[:count], refs[count : 2 * count]
    send, recv, local = refs[2 * count :]
    here = Place(n_mp)
    greet(here)

    def block(w, z, y, x, c, half=None):
        whole = wholes[w]
        depth = shards[w].shape[-2]
        start, size = z * depth, depth
        if half is not None:
            size = depth // 2
            start = start + half * size
        spot = (pl.ds(pl.multiple_of(start, 16), size), here.column(y, x, c))
        return whole.at[(slice(None),) + spot] if len(whole.shape) == 3 else whole.at[spot]

    y, x, c = here.y, here.x, here.c
    other_y, other_x, other_c = 1 - y, 1 - x, 1 - c
    started = []
    kept = []
    step = [0] * count

    def relay(w, source, spot, peer):
        index = step[w]
        step[w] += 1
        copy = push(source, spot, (send.at[w], recv.at[w]), index, peer)
        started.append(copy)
        return copy

    own, by_z, by_x, by_y = {}, {}, {}, {}
    for w in range(count):
        mine = block(w, here.z, y, x, c)
        keep = pltpu.make_async_copy(shards[w], mine, local.at[w])
        keep.start()
        kept.append(keep)
        by_z[w] = [relay(w, shards[w], mine, here.by_z(off)) for off in range(1, n_mp)]
        by_x[w] = [relay(w, shards[w], mine, here.by_x)]
        by_y[w] = [relay(w, shards[w], mine, here.by_y)]
        relay(w, shards[w], mine, here.by_core)
    for w in range(count):
        for off in range(1, n_mp):
            by_z[w][off - 1].wait_recv()
            z = here.up(n_mp - off)
            got = block(w, z, y, x, c)
            by_x[w].append(relay(w, got, got, here.by_x))
            by_y[w].append(relay(w, got, got, here.by_y))
            relay(w, got, got, here.by_core)
        far = []
        for off in range(n_mp):
            z = here.up(n_mp - off) if off else here.z
            by_x[w][off].wait_recv()
            got = block(w, z, y, other_x, c, 1)
            far.append((relay(w, got, got, here.by_y), z, 1))
            got = block(w, z, y, other_x, c)
            relay(w, got, got, here.by_core)
            by_y[w][off].wait_recv()
            got = block(w, z, other_y, x, c, 0)
            far.append((relay(w, got, got, here.by_x), z, 0))
            got = block(w, z, other_y, x, c)
            relay(w, got, got, here.by_core)
        own[w] = far
    for w in range(count):
        for copy, z, half in own[w]:
            copy.wait_recv()
            got = block(w, z, other_y, other_x, c, half)
            relay(w, got, got, here.by_core)
    for keep in kept:
        keep.wait()
    waited = set()
    for w in range(count):
        for copy in by_z[w] + by_x[w] + by_y[w] + [f[0] for f in own[w]]:
            waited.add(id(copy))
    for copy in started:
        if id(copy) not in waited:
            copy.wait_recv()
        copy.wait_send()


def gather_call(shards, n_mp, collective_id):
    count = len(shards)
    wholes = [
        jax.ShapeDtypeStruct(s.shape[:-2] + (s.shape[-2] * n_mp, s.shape[-1] * 8), BF)
        for s in shards
    ]
    copies = n_mp - 1 + 3 + 3 * (n_mp - 1) + 4 * n_mp + 2 * n_mp
    moved = 2 * sum(math.prod(s.shape) for s in wholes)
    return pl.pallas_call(
        functools.partial(gather_kernel, n_mp, count),
        out_shape=wholes,
        in_specs=[pl.BlockSpec(memory_space=pltpu.VMEM)] * count,
        out_specs=[pl.BlockSpec(memory_space=pl.ANY)] * count,
        scratch_shapes=[
            pltpu.SemaphoreType.DMA((count, copies)),
            pltpu.SemaphoreType.DMA((count, copies)),
            pltpu.SemaphoreType.DMA((count,)),
        ],
        compiler_params=pltpu.CompilerParams(
            collective_id=collective_id, has_side_effects=True, vmem_limit_bytes=16 << 20
        ),
        cost_estimate=pl.CostEstimate(flops=0, bytes_accessed=8 * moved, transcendentals=0),
        name=f"gather_{collective_id}",
    )(*shards)


def added(target, terms, rows):
    piece = min(rows, 128)

    def body(i, carry):
        at = pl.ds(pl.multiple_of(i * piece, piece), piece)
        total = terms[0][at, :].astype(F32)
        for term in terms[1:]:
            total = total + term[at, :].astype(F32)
        target[at, :] = total.astype(target.dtype)
        return carry

    lax.fori_loop(0, rows // piece, body, 0)


def reduce_kernel(n_mp, plan, *refs):
    count = len(plan)
    grads, sums = refs[:count], refs[count : 2 * count]
    rest = refs[2 * count :]
    buffers = [rest[8 * w : 8 * w + 8] for w in range(count)]
    send, recv, local = rest[8 * count :]
    here = Place(n_mp)
    greet(here)
    y, x, c = here.y, here.x, here.c
    half_wide = 4 * LANES
    mine = pl.ds(pl.multiple_of(c * half_wide, half_wide), half_wide)
    theirs = pl.ds(pl.multiple_of((1 - c) * half_wide, half_wide), half_wide)
    offs = [*range(1, n_mp), 0]
    chunks = []
    base = 0
    for w, depth in enumerate(plan):
        size = depth // 2
        for turn, off in enumerate(offs):
            for half in range(2):
                chunks.append((w, turn, off, half, size, base))
                base += 4
    copies = {}

    def stage_zero(q):
        w, turn, off, half, size, base = chunks[q]
        own, core_in = buffers[w][:2]
        at = 2 * turn + half
        start = here.up(off) * plan[w] + half * size
        row = pl.ds(pl.multiple_of(start, 8), size)
        sent = push(grads[w].at[row, theirs], core_in.at[at], (send, recv), base, here.by_core)
        kept = pltpu.make_async_copy(grads[w].at[row, mine], own.at[at], local.at[q])
        kept.start()
        copies[q, 0] = (sent, kept)

    def stage_one(q):
        w, turn, off, half, size, base = chunks[q]
        own, core_in, pair, pair_in = buffers[w][:4]
        at = 2 * turn + half
        sent, kept = copies[q, 0]
        kept.wait()
        sent.wait_recv()
        for by in range(2):
            for bx in range(2):
                spot = pl.ds((2 * by + bx) * LANES, LANES)
                near, far = (bx, by) if half == 0 else (by, bx)
                added(
                    pair.at[at, near, far],
                    [own.at[at, :, spot], core_in.at[at, :, spot]],
                    size,
                )
        away = 1 - x if half == 0 else 1 - y
        peer = here.by_x if half == 0 else here.by_y
        copies[q, 1] = push(pair.at[at, away], pair_in.at[at], (send, recv), base + 1, peer)

    def stage_two(q):
        w, turn, off, half, size, base = chunks[q]
        pair, pair_in, quad, quad_in = buffers[w][2:6]
        at = 2 * turn + half
        copies[q, 1].wait_recv()
        me = x if half == 0 else y
        for far in range(2):
            added(quad.at[at, far], [pair.at[at, me, far], pair_in.at[at, far]], size)
        away = 1 - y if half == 0 else 1 - x
        peer = here.by_y if half == 0 else here.by_x
        copies[q, 2] = push(quad.at[at, away], quad_in.at[at], (send, recv), base + 2, peer)

    def stage_three(q):
        w, turn, off, half, size, base = chunks[q]
        quad, quad_in, plane, plane_in = buffers[w][4:8]
        at = 2 * turn + half
        copies[q, 2].wait_recv()
        me = y if half == 0 else x
        added(plane.at[at], [quad.at[at, me], quad_in.at[at]], size)
        if off:
            copies[q, 3] = push(
                plane.at[at], plane_in.at[at], (send, recv), base + 3, here.by_z(off)
            )

    def stage_four(q):
        w, turn, off, half, size, base = chunks[q]
        plane, plane_in = buffers[w][6:8]
        first = q - 2 * (n_mp - 1)
        for k in range(n_mp - 1):
            copies[first + 2 * k, 3].wait_recv()
        terms = [plane_in.at[2 * k + half] for k in range(n_mp - 1)]
        added(
            sums[w].at[pl.ds(half * size, size)],
            [plane.at[2 * turn + half]] + terms,
            size,
        )

    total = len(chunks)
    for q in range(total):
        stage_zero(q)
    for q in range(total + 6):
        if q < total:
            stage_one(q)
        if 0 <= q - 2 < total:
            stage_two(q - 2)
        if 0 <= q - 4 < total:
            stage_three(q - 4)
    for q in range(total):
        if chunks[q][2] == 0:
            stage_four(q)
    for (q, stage), copy in copies.items():
        (copy[0] if stage == 0 else copy).wait_send()


def reduce_call(grads, n_mp, collective_id):
    plan = [g.shape[0] // n_mp for g in grads]
    scratch = []
    for g, depth in zip(grads, plan):
        n, size, dt = 2 * n_mp, depth // 2, g.dtype
        scratch += [
            pltpu.VMEM((n, size, 4 * LANES), dt),
            pltpu.VMEM((n, size, 4 * LANES), dt),
            pltpu.VMEM((n, 2, 2, size, LANES), dt),
            pltpu.VMEM((n, 2, size, LANES), dt),
            pltpu.VMEM((n, 2, size, LANES), dt),
            pltpu.VMEM((n, size, LANES), dt),
            pltpu.VMEM((n, size, LANES), dt),
            pltpu.VMEM((n - 2, size, LANES), dt),
        ]
    chunks = 2 * n_mp * len(grads)
    moved = sum(g.size * g.dtype.itemsize for g in grads)
    return pl.pallas_call(
        functools.partial(reduce_kernel, n_mp, plan),
        out_shape=[jax.ShapeDtypeStruct((depth, LANES), F32) for depth in plan],
        in_specs=[pl.BlockSpec(memory_space=pl.ANY)] * len(grads),
        out_specs=[pl.BlockSpec(memory_space=pltpu.VMEM)] * len(grads),
        scratch_shapes=scratch
        + [
            pltpu.SemaphoreType.DMA((4 * chunks,)),
            pltpu.SemaphoreType.DMA((4 * chunks,)),
            pltpu.SemaphoreType.DMA((chunks,)),
        ],
        compiler_params=pltpu.CompilerParams(
            collective_id=collective_id, has_side_effects=True, vmem_limit_bytes=58 << 20
        ),
        cost_estimate=pl.CostEstimate(flops=0, bytes_accessed=8 * moved, transcendentals=0),
        name=f"reduce_{collective_id}",
    )(*grads)


def spread_kernel(n_mp, part_ref, whole_ref, send, recv, local):
    here = Place(n_mp)
    greet(here)
    y, x, c = here.y, here.x, here.c
    own = pltpu.make_async_copy(part_ref, whole_ref.at[y, x, c, here.z], local)
    own.start()
    sems = (send, recv)
    sent = [
        push(part_ref, whole_ref.at[y, x, c, here.z], sems, off - 1, here.by_z(off))
        for off in range(1, n_mp)
    ]
    own.wait()
    for copy in sent:
        copy.wait_recv()
    line = whole_ref.at[y, x, c]
    sent.append(push(line, line, sems, n_mp - 1, here.by_x))
    sent.append(push(line, line, sems, n_mp, here.by_core))
    sent[-2].wait_recv()
    sent[-1].wait_recv()
    for spot in ((y, x, c), (y, 1 - x, c)):
        line = whole_ref.at[spot]
        sent.append(push(line, line, sems, len(sent), here.by_y))
    line = whole_ref.at[y, 1 - x, c]
    sent.append(push(line, line, sems, len(sent), here.by_core))
    sent[-3].wait_recv()
    sent[-2].wait_recv()
    first = len(sent)
    for bx in range(2):
        line = whole_ref.at[1 - y, bx, c]
        sent.append(push(line, line, sems, len(sent), here.by_core))
    for copy in sent[first - 1 :]:
        copy.wait_recv()
    for copy in sent:
        copy.wait_send()


def spread_call(part, n_mp, collective_id):
    copies = n_mp + 6
    return pl.pallas_call(
        functools.partial(spread_kernel, n_mp),
        out_shape=jax.ShapeDtypeStruct((2, 2, 2, n_mp) + part.shape, F32),
        in_specs=[pl.BlockSpec(memory_space=pltpu.VMEM)],
        out_specs=pl.BlockSpec(memory_space=pltpu.VMEM),
        scratch_shapes=[
            pltpu.SemaphoreType.DMA((copies,)),
            pltpu.SemaphoreType.DMA((copies,)),
            pltpu.SemaphoreType.DMA,
        ],
        compiler_params=pltpu.CompilerParams(
            collective_id=collective_id, has_side_effects=True
        ),
        name=f"spread_{collective_id}",
    )(part)


def by_core_first(values):
    split = values.reshape(values.shape[0], 4, 2, -1)
    return split.transpose(0, 2, 1, 3).reshape(values.shape)


def packed(small, group):
    flat = jnp.concatenate([s.reshape(-1) for s in small])
    wide = 8 * LANES
    count = -(-flat.size // (wide * group)) * group
    return jnp.pad(flat, (0, count * wide - flat.size)).reshape(count, wide)


def unpacked(matrix, like):
    flat, parts, at = matrix.reshape(-1), [], 0
    for s in like:
        parts.append(flat[at : at + s.size].reshape(s.shape))
        at += s.size
    return tuple(parts)


class KernelPaths:
    def __init__(self, n_mp):
        self.n_mp = n_mp

    def gather_mixer(self, in_shard, out_shard):
        return gather_call([in_shard, out_shard], self.n_mp, 1)

    def gather_ffn(self, up_shard, down_shard):
        return gather_call([up_shard, down_shard], self.n_mp, 2)

    def partial_grad(self, left, right, parts):
        if parts:
            left = left.reshape(left.shape[0], parts, self.n_mp, -1)
            left = left.transpose(0, 2, 1, 3).reshape(left.shape[0], -1)
        return lax.dot_general(
            left, by_core_first(right), COLS_COLS, preferred_element_type=F32
        ).astype(BF)

    def reduce_ffn(self, up_pair, down_pair):
        pair = [self.partial_grad(*up_pair), self.partial_grad(*down_pair)]
        return tuple(reduce_call(pair, self.n_mp, 3))

    def reduce_mixer(self, in_pair, out_pair, small, ffn_sums):
        matrix = packed(small, 16 * self.n_mp)
        grads = [
            self.partial_grad(*in_pair),
            self.partial_grad(*out_pair),
            by_core_first(matrix),
        ]
        in_sum, out_sum, small_part = reduce_call(grads, self.n_mp, 4)
        large = (in_sum, out_sum) + tuple(ffn_sums)
        mark = jnp.full((8, LANES), squares(large))
        part = jnp.concatenate([small_part, mark], axis=0)
        whole = spread_call(part, self.n_mp, 5)
        depth = small_part.shape[0]
        total_large = jnp.sum(whole[..., depth, 0])
        matrix = whole[..., :depth, :].transpose(3, 4, 0, 1, 2, 5).reshape(matrix.shape)
        sums = unpacked(matrix, small)
        depth = in_sum.shape[0] // in_pair[2]
        in_sum = in_sum.reshape(in_pair[2], depth, LANES)
        return sums + (in_sum,) + large[1:], total_large + squares(sums)


def choose_paths(mesh):
    if mesh.shape["dp"] == 8 and mesh.shape["mp"] == 4:
        return KernelPaths(mesh.shape["mp"])
    return PlainPaths()


def solution(mesh):
    tokens = P(("dp", "mp"), None)
    weights = (P(None, "mp", "dp"),) * 3 + (P("mp", "dp"),) * 9
    return jax.shard_map(
        functools.partial(per_device, choose_paths(mesh)),
        mesh=mesh,
        in_specs=(tokens, tokens, P("dp"), P()) + (P(),) * 18 + weights,
        out_specs=(tokens, tokens, P()) + (P(),) * 18 + weights,
        check_vma=False,
    )
```
